32 devices in a mesh: dp: 8 (over y, x, core), expert: 4 (over z).
Axes of the slice: x: 2, y: 2, z: 4, core: 2. Of those that a mesh axis runs over, the one named last changes fastest.
Arguments:
- tokens: bfloat16 [4096, 2048], P(('dp', 'expert')), may hold values from -6 to 6
- cotangent: bfloat16 [4096, 2048], P(('dp', 'expert')), may hold values from -6 to 6
- expert_ids: int32 [4096, 2], P(('dp', 'expert')), may hold values from 0 to 3, all different within a row; in each aligned block of 128 rows (0 to 127, 128 to 255, ...) at most 128 rows name the same one
- combine: float32 [4096, 2], P(('dp', 'expert')), may hold values from 0.1 to 1
- w_gate: bfloat16 [4, 2048, 768], P('expert'), may hold values from -0.125 to 0.125
- w_up: bfloat16 [4, 2048, 768], P('expert'), may hold values from -0.125 to 0.125
- w_down: bfloat16 [4, 768, 2048], P('expert'), may hold values from -0.21875 to 0.21875
Outputs:
- input_grad: bfloat16 [4096, 2048], P(('dp', 'expert'))
- combine_grad: float32 [4096, 2], P(('dp', 'expert'))
- gate_grad: bfloat16 [4, 2048, 768], P('expert', 'dp')
- up_grad: bfloat16 [4, 2048, 768], P('expert', 'dp')
- down_grad: bfloat16 [4, 768, 2048], P('expert', 'dp')
The draws below stay inside these ranges and needn't reach their ends.
Inputs may be any that keep to these rules, and one draw needn't show every extreme that they name: `expert_ids`: each token names 2 different experts. In the rows of one device no expert is named by more than 128 tokens, and in some devices' rows some expert is named by exactly 128.
All inputs are finite; a program needn't handle non-finite values.
Results may differ from the reference program's by a relative error of at most 0.02.
Values may be sent and summed in bfloat16 or wider, within the bound.
A program may use at most 128 MiB of HBM per device.

```python
import math
import jax
import jax.numpy as jnp
import numpy as np
from jax import lax

D = 2048
FF = 768
TOK_DEV = 128
TOP = 2
EXPERTS = 4
CAP = 128
TOKENS = 4096
N_DP = 8
N_EXPERT = 4


def steps_of(own_key, shape, split, smallest, largest):
    gain, own = 1.0, jax.random.fold_in(own_key, 6)
    for axis_at, parts in split:
        heights = jnp.exp(jax.random.uniform(jax.random.fold_in(own, axis_at), (parts,), jnp.float32, smallest / len(split), largest / len(split)))
        gain = gain * jnp.repeat(heights, shape[axis_at] // parts).reshape([-1 if axis == axis_at else 1 for axis in range(len(shape))])
    return gain


def deal_out(own_key, own, number, rows, number_of, top, bound, skew):
    ranking = jax.random.permutation(own_key, number_of)
    crowded, common = load_shares(number_of, rows * top, bound, skew, True), load_shares(number_of, rows * top, bound, skew, False)
    places = jnp.arange(number_of)

    def named(lengths, offset_by):
        used = int((lengths > 0).sum())
        fixed = max(1, used // 4)
        shifted = fixed + (places - fixed + offset_by * (used - fixed)) % max(1, number_of - fixed)
        return jnp.zeros((number_of,), jnp.int32).at[ranking[jnp.where(places < fixed, places, shifted)]].set(jnp.asarray(lengths, jnp.int32))

    lengths = jnp.where(number % 4 == 0, named(crowded, number // 4), named(common, number - number // 4 - 1))
    mixed = jax.random.permutation(jax.random.fold_in(own, 3), number_of)
    donor, taker = mixed[0:number_of // 2 * 2:2], mixed[1:number_of // 2 * 2:2]
    room = jnp.minimum(lengths[donor] - 1, bound - lengths[taker]) // 2
    room = jnp.where((donor == ranking[0]) | (taker == ranking[0]) | (lengths[taker] == 0), 0, jnp.maximum(room, 0))
    shifted = jax.random.randint(jax.random.fold_in(own, 4), (number_of // 2,), 0, 1 << 20) % (room + 1)
    lengths = lengths.at[donor].add(-shifted).at[taker].add(shifted)
    items = jnp.searchsorted(jnp.cumsum(lengths), jnp.arange(rows * top), side="right").astype(jnp.int32)
    listing = items.reshape(top, rows).T
    listing = listing[jax.random.permutation(jax.random.fold_in(own, 1), rows)]
    offset_by = jax.random.randint(jax.random.fold_in(own, 2), (rows, 1), 0, top)
    return jnp.take_along_axis(listing, (jnp.arange(top)[None, :] + offset_by) % top, axis=1)


def load_shares(number_of, total, bound, skew, full):
    weights = [(1 << 20) // math.isqrt(standing ** skew) + 1 for standing in range(1, number_of + 1)]
    largest = bound if full else min(bound, max(-(-total // number_of), total * weights[0] // sum(weights)))
    least = 1 if total - largest >= number_of - 1 else 0
    holding, spare = [largest] + [least] * (number_of - 1), total - largest - least * (number_of - 1)
    while spare > 0:
        candidates = [i for i in range(1, number_of) if holding[i] < largest] or [i for i in range(1, number_of) if holding[i] < bound]
        mass, left = sum([weights[i] for i in candidates]), spare
        for i in candidates:
            more = min(bound - holding[i], max(1, left * weights[i] // mass), spare)
            holding[i] = holding[i] + more
            spare = spare - more
    return np.array(holding)


def noise(rng, shape, deviation, reach, split=(), kind=jnp.bfloat16):
    result = jax.random.normal(rng, shape, jnp.float32) * deviation
    if len(split) > 0:
        result = steps_of(rng, shape, split, -0.22, 0.18) * result
    return jnp.clip(result, min=-reach, max=reach).astype(kind)


def setup_inputs(seed: int = 0) -> dict:
    key_list = jax.random.split(jax.random.key(seed), 8)
    tokens = noise(key_list[0], (TOKENS, D), 1.0, 6.0, ((0, 32),))
    cotangent = noise(key_list[1], (TOKENS, D), 1.0, 6.0, ((0, 32),))
    expert_ids_keys = jax.random.split(jax.random.fold_in(key_list[2], 1), TOKENS // TOK_DEV)
    expert_ids_turns = jax.random.permutation(jax.random.fold_in(key_list[2], 3), TOKENS // TOK_DEV)
    expert_ids = jax.vmap(lambda own, number: deal_out(jax.random.fold_in(key_list[2], 2), own, number, TOK_DEV, EXPERTS, TOP, CAP, 2))(expert_ids_keys, expert_ids_turns).reshape((TOKENS, TOP))
    combine = jnp.clip(jnp.exp(math.log(1.0) - 2.3025851 * jax.random.uniform(key_list[3], (TOKENS, TOP), jnp.float32) ** steps_of(key_list[3], (TOKENS, TOP), ((0, 32),), -0.2, 0.2)), 0.1, 1.0)
    w_gate = noise(key_list[4], (EXPERTS, D, FF), D ** -0.5, 0.125, ((0, 4),))
    w_up = noise(key_list[5], (EXPERTS, D, FF), D ** -0.5, 0.125, ((0, 4),))
    w_down = noise(key_list[6], (EXPERTS, FF, D), FF ** -0.5, 0.21875, ((0, 4),))
    return dict(tokens=tokens, cotangent=cotangent, expert_ids=expert_ids, combine=combine, w_gate=w_gate, w_up=w_up, w_down=w_down)


def slot_table(expert_ids, experts_all, capacity):
    pairs = expert_ids.reshape(-1).astype(jnp.int32)
    count = pairs.shape[0]
    onehot = (pairs[:, None] == jnp.arange(experts_all, dtype=jnp.int32)[None, :]).astype(jnp.int32)
    before = jnp.cumsum(onehot, axis=0) - onehot
    position = jnp.sum(before * onehot, axis=1).astype(jnp.int32)
    dest = (pairs * capacity + position).astype(jnp.int32)
    filled = jnp.zeros((experts_all * capacity,), jnp.int32).at[dest].set(jnp.arange(count, dtype=jnp.int32) + 1)
    return dest, filled


def gather_rows(tokens, cotangent, combine, filled, top):
    live = filled > 0
    pair = jnp.maximum(filled - 1, 0).astype(jnp.int32)
    source = (pair // top).astype(jnp.int32)
    rows_x = jnp.where(live[:, None], jnp.take(tokens, source, axis=0), jnp.zeros((), tokens.dtype))
    rows_dy = jnp.where(live[:, None], jnp.take(cotangent, source, axis=0), jnp.zeros((), cotangent.dtype))
    rows_c = jnp.where(live, jnp.take(combine.reshape(-1), pair, axis=0), jnp.zeros((), combine.dtype))
    return rows_x, rows_dy, rows_c


def forward_part(rows_x, gate_mat, up_mat, down_mat):
    gate = jnp.dot(rows_x, gate_mat, preferred_element_type=jnp.float32)
    up = jnp.dot(rows_x, up_mat, preferred_element_type=jnp.float32)
    sig = jax.nn.sigmoid(gate)
    act = gate * sig
    hidden = (act * up).astype(jnp.bfloat16)
    output = jnp.dot(hidden, down_mat, preferred_element_type=jnp.float32)
    return gate, up, sig, act, hidden, output


def backward_part(state, rows_dy, rows_c, gate_mat, up_mat, down_mat):
    gate, up, sig, act, hidden, output = state
    comb_grad = jnp.sum(rows_dy.astype(jnp.float32) * output, axis=1)
    scaled = (rows_c[:, None] * rows_dy.astype(jnp.float32)).astype(jnp.bfloat16)
    last = (((1,), (1,)), ((), ()))
    hidden_grad = lax.dot_general(scaled, down_mat, last, preferred_element_type=jnp.float32)
    gate_d = (hidden_grad * up * (sig * (1.0 + gate * (1.0 - sig)))).astype(jnp.bfloat16)
    up_d = (hidden_grad * act).astype(jnp.bfloat16)
    row_grad = lax.dot_general(gate_d, gate_mat, last, preferred_element_type=jnp.float32)
    row_grad = (row_grad + lax.dot_general(up_d, up_mat, last, preferred_element_type=jnp.float32)).astype(jnp.bfloat16)
    return comb_grad, scaled, gate_d, up_d, row_grad


def reference(tokens, cotangent, expert_ids, combine, w_gate, w_up, w_down):
    first = (((0,), (0,)), ((), ()))
    x_all = tokens.reshape(N_DP, N_EXPERT, TOK_DEV, D)
    dy_all = cotangent.reshape(N_DP, N_EXPERT, TOK_DEV, D)
    id_all = expert_ids.reshape(N_DP, N_EXPERT, TOK_DEV, TOP)
    c_all = combine.reshape(N_DP, N_EXPERT, TOK_DEV, TOP)

    def prepare(x_q, dy_q, id_q, c_q):
        dest, filled = slot_table(id_q, EXPERTS, CAP)
        rows_x, rows_dy, rows_c = gather_rows(x_q, dy_q, c_q, filled, TOP)
        return dest, rows_x.reshape(EXPERTS, CAP, D), rows_dy.reshape(EXPERTS, CAP, D), rows_c.reshape(EXPERTS, CAP)

    def one_expert(item):
        inputs, cot_rows, comb_rows, gate_mat, up_mat, down_mat = item
        state = forward_part(inputs, gate_mat, up_mat, down_mat)
        comb_grad, scaled, gate_d, up_d, row_grad = backward_part(state, cot_rows, comb_rows, gate_mat, up_mat, down_mat)
        gate_part = lax.dot_general(inputs, gate_d, first, preferred_element_type=jnp.float32).astype(jnp.bfloat16)
        up_part = lax.dot_general(inputs, up_d, first, preferred_element_type=jnp.float32).astype(jnp.bfloat16)
        down_part = lax.dot_general(state[4], scaled, first, preferred_element_type=jnp.float32).astype(jnp.bfloat16)
        return row_grad, comb_grad, gate_part, up_part, down_part

    def finish(flat_rows, flat_comb, dest):
        picked = jnp.take(flat_rows, dest, axis=0).reshape(TOK_DEV, TOP, D)
        summed = jnp.sum(picked.astype(jnp.float32), axis=1).astype(jnp.bfloat16)
        return summed, jnp.take(flat_comb, dest, axis=0).reshape(TOK_DEV, TOP)

    def one_replica(carry, inputs):
        x_r, dy_r, id_r, c_r = inputs
        dest, rx, rdy, rc = jax.vmap(prepare)(x_r, dy_r, id_r, c_r)
        group_x = jnp.transpose(rx, (1, 0, 2, 3)).reshape(EXPERTS, N_EXPERT * CAP, D)
        group_dy = jnp.transpose(rdy, (1, 0, 2, 3)).reshape(EXPERTS, N_EXPERT * CAP, D)
        group_c = jnp.transpose(rc, (1, 0, 2)).reshape(EXPERTS, N_EXPERT * CAP)
        rows, combs, gate_part, up_part, down_part = lax.map(one_expert, (group_x, group_dy, group_c, w_gate, w_up, w_down))
        gate_part, up_part, down_part = lax.optimization_barrier((gate_part, up_part, down_part))
        carry = (carry[0] + gate_part.astype(jnp.float32), carry[1] + up_part.astype(jnp.float32), carry[2] + down_part.astype(jnp.float32))
        back = jnp.transpose(rows.reshape(EXPERTS, N_EXPERT, CAP, D), (1, 0, 2, 3)).reshape(N_EXPERT, EXPERTS * CAP, D)
        back_c = jnp.transpose(combs.reshape(EXPERTS, N_EXPERT, CAP), (1, 0, 2)).reshape(N_EXPERT, EXPERTS * CAP)
        grads_in, grads_c = jax.vmap(finish)(back, back_c, dest)
        return carry, (grads_in, grads_c)

    start = (jnp.zeros((EXPERTS, D, FF), jnp.float32), jnp.zeros((EXPERTS, D, FF), jnp.float32), jnp.zeros((EXPERTS, FF, D), jnp.float32))
    sums, (grads_in, grads_c) = lax.scan(one_replica, start, (x_all, dy_all, id_all, c_all))
    input_grad = grads_in.reshape(TOKENS, D)
    combine_grad = grads_c.reshape(TOKENS, TOP)
    return (input_grad, combine_grad, sums[0].astype(jnp.bfloat16), sums[1].astype(jnp.bfloat16), sums[2].astype(jnp.bfloat16))
```

```python
import jax
import jax.numpy as jnp
from jax import lax
from jax.sharding import PartitionSpec as P


def shards(tokens, cotangent, expert_ids, combine, w_gate, w_up, w_down):
    first = (((0,), (0,)), ((), ()))
    last = (((1,), (1,)), ((), ()))
    local = w_gate.shape[0]
    groups = lax.axis_size("expert")
    experts = local * groups
    rows, top = expert_ids.shape
    hidden_width = w_gate.shape[2]
    names = jnp.arange(experts, dtype=jnp.int32)
    hits = expert_ids[:, :, None] == names
    weight = jnp.sum(jnp.where(hits, combine[:, :, None], 0.0), axis=1)
    weight = lax.all_to_all(weight, "expert", split_axis=1, concat_axis=0, tiled=True)
    x = lax.all_gather(tokens, "expert", axis=0, tiled=True)
    dy = lax.all_gather(cotangent, "expert", axis=0, tiled=True)
    row_sum = 0.0
    combs, gates, ups, downs = [], [], [], []
    for i in range(local):
        w_g, w_u, w_d = w_gate[i], w_up[i], w_down[i]
        gate = jnp.dot(x, w_g, preferred_element_type=jnp.float32)
        up = jnp.dot(x, w_u, preferred_element_type=jnp.float32)
        sig = jax.nn.sigmoid(gate)
        act = gate * sig
        hidden = (act * up).astype(jnp.bfloat16)
        scaled = (weight[:, i : i + 1] * dy.astype(jnp.float32)).astype(jnp.bfloat16)
        output = jnp.dot(hidden, w_d, preferred_element_type=jnp.float32)
        combs.append(jnp.sum(dy.astype(jnp.float32) * output, axis=1))
        hidden_grad = lax.dot_general(scaled, w_d, last, preferred_element_type=jnp.float32)
        gate_d = (hidden_grad * up * (sig * (1.0 + gate * (1.0 - sig)))).astype(jnp.bfloat16)
        up_d = (hidden_grad * act).astype(jnp.bfloat16)
        row = lax.dot_general(gate_d, w_g, last, preferred_element_type=jnp.float32)
        row = row + lax.dot_general(up_d, w_u, last, preferred_element_type=jnp.float32)
        row_sum = row_sum + row.astype(jnp.bfloat16).astype(jnp.float32)
        downs.append(lax.dot_general(hidden, scaled, first, preferred_element_type=jnp.float32))
        gates.append(lax.dot_general(x, gate_d, first, preferred_element_type=jnp.float32))
        ups.append(lax.dot_general(x, up_d, first, preferred_element_type=jnp.float32))

    def reduced(parts):
        return jnp.stack(
            [
                lax.psum_scatter(part.astype(jnp.bfloat16), "dp", scatter_dimension=0, tiled=True)
                for part in parts
            ]
        )

    down_grad = reduced(downs)
    gate_grad = reduced(gates)
    up_grad = reduced(ups)
    input_grad = lax.psum_scatter(
        row_sum.astype(jnp.bfloat16), "expert", scatter_dimension=0, tiled=True
    )
    comb = jnp.stack(combs)
    comb = lax.all_to_all(comb, "expert", split_axis=1, concat_axis=0, tiled=True)
    combine_grad = jnp.sum(jnp.where(hits, comb.T[:, None, :], 0.0), axis=2)
    return (input_grad, combine_grad, gate_grad, up_grad, down_grad)


def solution(mesh):
    by_token = P(("dp", "expert"), None)
    by_expert = P("expert", None, None)
    by_row = P("expert", "dp", None)
    return jax.shard_map(
        shards,
        mesh=mesh,
        in_specs=(by_token,) * 4 + (by_expert,) * 3,
        out_specs=(by_token, by_token, by_row, by_row, by_row),
        check_vma=False,
    )
```

```python
import functools
import jax
import jax.numpy as jnp
from jax import lax
from jax.experimental import pallas as pl
from jax.experimental.pallas import tpu as pltpu
from jax.sharding import PartitionSpec as P

MESH = pl.DeviceIdType.MESH
VMEM = pl.BlockSpec(memory_space=pltpu.VMEM)
LIMIT = 56 * 1024 * 1024


def remote(src, dst, send, recv, axis, target):
    return pltpu.make_async_remote_copy(
        src_ref=src,
        dst_ref=dst,
        send_sem=send,
        recv_sem=recv,
        device_id={axis: target},
        device_id_type=MESH,
    )


def gather_kernel(n, x, dy, w, x_all, dy_all, w_all, send, recv, w_send, w_recv):
    me = lax.axis_index("expert")
    barrier = pltpu.get_barrier_semaphore()
    for k in range(1, n):
        pl.semaphore_signal(
            barrier, inc=1, device_id={"expert": lax.rem(me + k, n)}, device_id_type=MESH
        )
    pl.semaphore_wait(barrier, n - 1)

    def hop(t, side, s):
        own, full = ((x, x_all), (dy, dy_all))[t]
        step = 1 if side == 0 else -1
        block = jnp.clip(me - step * s, 0, n - 1)
        src = own if s == 0 else full.at[block]
        target = jnp.clip(me + step, 0, n - 1)
        return remote(
            src, full.at[block], send.at[t, side, s], recv.at[t, side, s], "expert", target
        )

    def arrival(t, side, s):
        full = (x_all, dy_all)[t]
        step = 1 if side == 0 else -1
        block = jnp.clip(me - step * (s + 1), 0, n - 1)
        slot = full.at[block]
        return remote(slot, slot, send.at[t, side, s], recv.at[t, side, s], "expert", me)

    def sends(side, s):
        if side == 0:
            return jnp.logical_and(me >= s, me + 1 < n)
        return jnp.logical_and(me + s < n, me >= 1)

    def gets(side, s):
        return me >= s + 1 if side == 0 else me + s + 1 < n

    for t in range(2):
        for s in range(n):
            for side in range(2):
                if s >= 1:

                    @pl.when(gets(side, s - 1))
                    def _():
                        arrival(t, side, s - 1).wait_recv()

                if s < n - 1:

                    @pl.when(sends(side, s))
                    def _():
                        hop(t, side, s).start()

            if s == 0:
                if t == 0:
                    small = []
                    for k in range(1, n):
                        small.append(
                            remote(
                                w,
                                w_all.at[k],
                                w_send.at[k],
                                w_recv.at[k],
                                "expert",
                                lax.rem(me + k, n),
                            )
                        )
                        small[-1].start()
                    x_all[me] = x[...]
                    dy_all[me] = dy[...]
                    w_all[0] = w[...]
    for t in range(2):
        for s in range(n - 1):
            for side in range(2):

                @pl.when(sends(side, s))
                def _():
                    hop(t, side, s).wait_send()

    for copy in small:
        copy.wait()


def gather_all(n, x, dy, w):
    outs = [jax.ShapeDtypeStruct((n,) + a.shape, a.dtype) for a in (x, dy, w)]
    return pl.pallas_call(
        functools.partial(gather_kernel, n),
        out_shape=outs,
        in_specs=[VMEM] * 3,
        out_specs=[VMEM] * 3,
        scratch_shapes=[
            pltpu.SemaphoreType.DMA((2, 2, n)),
            pltpu.SemaphoreType.DMA((2, 2, n)),
            pltpu.SemaphoreType.DMA((n,)),
            pltpu.SemaphoreType.DMA((n,)),
        ],
        compiler_params=pltpu.CompilerParams(
            collective_id=0, has_side_effects=True, vmem_limit_bytes=LIMIT
        ),
        name="gather_all",
    )(x, dy, w)


def reduce_kernel(n, bits, *refs):
    rows, comb, both, down, in_grad, comb_all, gate_out, up_out, down_out = refs[:9]
    got_rows, r_send, r_recv, c_send, c_recv = refs[9:14]
    rest = refs[14:]
    gots = [rest[2 * p : 2 * p + 2] for p in range(bits)]
    sums = [rest[2 * bits + 2 * p : 2 * bits + 2 * p + 2] for p in range(bits - 1)]
    send, recv = rest[-2:]
    me = lax.axis_index("expert")
    rank = lax.axis_index("dp")
    bit = [lax.rem(rank // (1 << b), 2) for b in range(bits)]
    mate = [rank + (1 - 2 * bit[b]) * (1 << b) for b in range(bits)]
    barrier = pltpu.get_barrier_semaphore()
    for k in range(1, n):
        pl.semaphore_signal(
            barrier, inc=1, device_id={"expert": lax.rem(me + k, n)}, device_id_type=MESH
        )
    for b in range(bits):
        pl.semaphore_signal(barrier, inc=1, device_id={"dp": mate[b]}, device_id_type=MESH)
    pl.semaphore_wait(barrier, n - 1 + bits)

    orders = ([0] + list(range(1, bits)), [0] + list(range(bits - 1, 0, -1)))
    inputs = (both, down)

    def span(a, h):
        half = inputs[a].shape[2] // 2
        return pl.ds(h * half, half)

    def block_of(order, value, m):
        block = value * (1 << order[0])
        for i, b in enumerate(order[1:]):
            block = block + lax.rem(m // (1 << i), 2) * (1 << b)
        return block

    def copy(p, h, a, m):
        order = orders[h]
        b = order[p]
        if p == 0:
            src = inputs[a].at[block_of(order, 1 - bit[b], m), :, span(a, h)]
        else:
            src = sums[p - 1][a].at[h, 1 - bit[b] + 2 * m]
        return remote(
            src, gots[p][a].at[h, m], send.at[p, h, a, m], recv.at[p, h, a, m], "dp", mate[b]
        )

    def slots(p, h):
        count = 1 << (bits - 1 - p)
        if count == 1:
            return [(0, None)]
        lead = bit[orders[h][p + 1]]
        going = [(1 - lead + 2 * k, k) for k in range(count // 2)]
        return going + [(lead + 2 * k, None) for k in range(count // 2)]

    for h in range(2):
        for m, _ in slots(0, h):
            for a in range(2):
                copy(0, h, a, m).start()
    exchange = []
    for k in range(1, n):
        target = lax.rem(me + k, n)
        exchange.append(
            remote(rows.at[target], got_rows.at[k], r_send.at[k], r_recv.at[k], "expert", target)
        )
        exchange.append(
            remote(comb.at[target], comb_all.at[k], c_send.at[k], c_recv.at[k], "expert", target)
        )
    for item in exchange:
        item.start()
    comb_all[0] = comb[me]

    for p in range(bits):
        plans = [slots(p, h) for h in range(2)]
        for i in range(len(plans[0])):
            for h in range(2):
                m, onward = plans[h][i]
                order = orders[h]
                mine = bit[order[p]]
                for a in range(2):
                    copy(p, h, a, m).wait_recv()
                    if p == 0:
                        held = inputs[a][block_of(order, mine, m), :, span(a, h)]
                    else:
                        held = sums[p - 1][a][h, mine + 2 * m]
                    total = held.astype(jnp.float32) + gots[p][a][h, m].astype(jnp.float32)
                    total = total.astype(jnp.bfloat16)
                    if p < bits - 1:
                        sums[p][a][h, m] = total
                        if onward is not None:
                            copy(p + 1, h, a, onward).start()
                    elif a == 0:
                        (gate_out, up_out)[h][...] = total
                    else:
                        down_out[:, span(a, h)] = total
    for item in exchange:
        item.wait_recv()
    summed = rows[me].astype(jnp.float32)
    for k in range(1, n):
        summed = summed + got_rows[k].astype(jnp.float32)
    in_grad[...] = summed.astype(jnp.bfloat16)
    for item in exchange:
        item.wait_send()
    for p in range(bits):
        for h in range(2):
            for m, _ in slots(p, h):
                for a in range(2):
                    copy(p, h, a, m).wait_send()


def reduce_all(n, replicas, rows, comb, both, down):
    bits = replicas.bit_length() - 1
    width = both.shape[2] // 2
    bf16 = jnp.bfloat16
    outs = [
        jax.ShapeDtypeStruct(rows.shape[1:], bf16),
        jax.ShapeDtypeStruct(comb.shape, jnp.float32),
        jax.ShapeDtypeStruct((both.shape[1], width), bf16),
        jax.ShapeDtypeStruct((both.shape[1], width), bf16),
        jax.ShapeDtypeStruct(down.shape[1:], bf16),
    ]
    halves = [(a.shape[1], a.shape[2] // 2) for a in (both, down)]
    scratch = [pltpu.VMEM(rows.shape, bf16)]
    scratch += [pltpu.SemaphoreType.DMA((n,))] * 4
    for phases in (bits, bits - 1):
        for p in range(phases):
            scratch += [pltpu.VMEM((2, 1 << (bits - 1 - p)) + half, bf16) for half in halves]
    scratch += [pltpu.SemaphoreType.DMA((bits, 2, 2, 1 << (bits - 1)))] * 2
    return pl.pallas_call(
        functools.partial(reduce_kernel, n, bits),
        out_shape=outs,
        in_specs=[VMEM] * 4,
        out_specs=[VMEM] * 5,
        scratch_shapes=scratch,
        compiler_params=pltpu.CompilerParams(
            collective_id=1, has_side_effects=True, vmem_limit_bytes=LIMIT
        ),
        name="reduce_all",
    )(rows, comb, both, down)


def shards(tokens, cotangent, expert_ids, combine, w_gate, w_up, w_down):
    first = (((0,), (0,)), ((), ()))
    last = (((1,), (1,)), ((), ()))
    groups = lax.axis_size("expert")
    replicas = lax.axis_size("dp")
    me = lax.axis_index("expert")
    rows, top = expert_ids.shape
    feature = tokens.shape[1]
    hidden_width = w_gate.shape[2]
    names = jnp.arange(groups, dtype=jnp.int32)
    hits = expert_ids[:, :, None] == names
    weight = jnp.sum(jnp.where(hits, combine[:, :, None], 0.0), axis=1)
    table = jnp.pad(weight.T, ((0, -groups % 8), (0, 0)))
    x, dy, tables = gather_all(groups, tokens, cotangent, table)
    x = x.reshape(groups * rows, feature)
    dy = dy.reshape(groups * rows, feature)
    sources = lax.rem(me - names + groups, groups)
    mine = lax.dynamic_index_in_dim(tables, me, axis=1, keepdims=False)
    coeff = mine[sources].reshape(groups * rows, 1)
    w_g, w_u, w_d = w_gate[0], w_up[0], w_down[0]
    gate = jnp.dot(x, w_g, preferred_element_type=jnp.float32)
    up = jnp.dot(x, w_u, preferred_element_type=jnp.float32)
    sig = jax.nn.sigmoid(gate)
    act = gate * sig
    hidden = (act * up).astype(jnp.bfloat16)
    scaled = (coeff * dy.astype(jnp.float32)).astype(jnp.bfloat16)
    output = jnp.dot(hidden, w_d, preferred_element_type=jnp.float32)
    comb = jnp.sum(dy.astype(jnp.float32) * output, axis=1)
    hidden_grad = lax.dot_general(scaled, w_d, last, preferred_element_type=jnp.float32)
    gate_d = (hidden_grad * up * (sig * (1.0 + gate * (1.0 - sig)))).astype(jnp.bfloat16)
    up_d = (hidden_grad * act).astype(jnp.bfloat16)
    row = lax.dot_general(gate_d, w_g, last, preferred_element_type=jnp.float32)
    row = row + lax.dot_general(up_d, w_u, last, preferred_element_type=jnp.float32)
    row = row.astype(jnp.bfloat16).reshape(groups, rows, feature)
    paired = jnp.concatenate([gate_d, up_d], axis=1)
    both = lax.dot_general(x, paired, first, preferred_element_type=jnp.float32)
    both = both.astype(jnp.bfloat16).reshape(replicas, feature // replicas, 2 * hidden_width)
    down = lax.dot_general(hidden, scaled, first, preferred_element_type=jnp.float32)
    down = down.astype(jnp.bfloat16).reshape(replicas, hidden_width // replicas, feature)
    comb = jnp.broadcast_to(comb.reshape(groups, 1, rows), (groups, 8, rows))
    input_grad, combs, gate_grad, up_grad, down_grad = reduce_all(
        groups, replicas, row, comb, both, down
    )
    comb = combs[sources, 0]
    combine_grad = jnp.sum(jnp.where(hits, comb.T[:, None, :], 0.0), axis=2)
    return (input_grad, combine_grad, gate_grad[None], up_grad[None], down_grad[None])


def solution(mesh):
    by_token = P(("dp", "expert"), None)
    by_expert = P("expert", None, None)
    by_row = P("expert", "dp", None)
    return jax.shard_map(
        shards,
        mesh=mesh,
        in_specs=(by_token,) * 4 + (by_expert,) * 3,
        out_specs=(by_token, by_token, by_row, by_row, by_row),
        check_vma=False,
    )
```
